32 devices in a mesh: rows: 8 (over z, x), grp: 4 (over y, core).
Axes of the slice: x: 2, y: 2, z: 4, core: 2. Of those that a mesh axis runs over, the one named last changes fastest.
Arguments:
- tile_values: bfloat16 [1024, 16, 128], P('rows'), may hold values from 0.049804688 to 1
- tile_ids: int32 [1024, 16], P('rows'), may hold values from 0 to 255, as said below
- doc_tiles: int32 [1024], P('rows'), may hold values from 1 to 16
- row_counts: int32 [8], replicated, may hold values from 1 to 128, 512 in all
Outputs:
- similarity: float32 [512, 512], P('rows', 'grp')
The draws below stay inside these ranges and needn't reach their ends.
Inputs may be any that keep to these rules, and one draw needn't show every extreme that they name: `row_counts`: the entries sum to 512. `tile_ids`: the 16 entries of a row are distinct.
All inputs are finite; a program needn't handle non-finite values.
Results may differ from the reference program's by a relative error of at most 0.0003.
Values may be sent and summed in bfloat16 or wider, within the bound.
A program may use at most 64 MiB of HBM per device.

```python
import math
import jax
import jax.numpy as jnp
import numpy as np
from jax import lax

VOCAB = 32768
TILE = 128
LTILES = 16
DOC_DEV = 64
PANELS = 8
CAP = 128
DOCS = 512
N_ROWS = 8


def draw_doc_tiles(key, part):
    first_key, second_key = jax.random.split(jax.random.fold_in(key, 11))
    first_draw = jax.random.randint(first_key, (PANELS * CAP,), 1, LTILES + 1)
    second_draw = jax.random.randint(second_key, (PANELS * CAP,), 1, LTILES + 1)
    return jnp.maximum(first_draw, second_draw).astype(jnp.int32)


def draw_tile_ids(key, part):
    tile_count = VOCAB // TILE
    noise = jax.random.randint(jax.random.fold_in(key, 23), (PANELS * CAP, tile_count), 0, 4096)
    tile_rank = jnp.arange(tile_count, dtype=jnp.int32)
    scores = noise * (tile_rank + 8) * tile_count + tile_rank
    order = jnp.argsort(scores, axis=1)
    return order[:, :LTILES].astype(jnp.int32)


def level_of(stream_key, dims, cuts, least, top_value):
    def one(dim, parts):
        steps = jax.random.uniform(jax.random.fold_in(jax.random.fold_in(stream_key, 6), dim), (parts,), jnp.float32, least / len(cuts), top_value / len(cuts))
        return jnp.repeat(jnp.exp(steps), dims[dim] // parts).reshape((-1,) + (1,) * (len(dims) - dim - 1))

    level = one(*cuts[0])
    for cut in cuts[1:]:
        level = level * one(*cut)
    return level


def length_profile(amount, total, most, lean):
    loads = [(1 << 20) // math.isqrt(grade ** lean) + 1 for grade in range(2, amount + 1)]
    spare, given = total - most - (amount - 1), [1] * (amount - 1)
    while spare > 0:
        movable = [i for i in range(amount - 1) if given[i] < most]
        whole, left = sum([loads[i] for i in movable]), spare
        for i in movable:
            addition = min(most - given[i], max(1, left * loads[i] // whole), spare)
            given[i] = given[i] + addition
            spare = spare - addition
    return np.array([most] + given)


def uneven_parts(key, number_of, total, most, skew):
    if number_of == 2:
        one = jax.random.randint(key, (), max(1, total - most), min(most, total - 1) + 1)
        return jnp.stack([one, total - one])
    tallies = jnp.asarray(length_profile(number_of, total, most, skew), jnp.int32)
    couples = (number_of - 1) // 2
    source_of, sink = tallies[1:1 + 2 * couples:2], tallies[2:2 + 2 * couples:2]
    room = jnp.minimum(source_of - 1, most - sink)
    shifted = jax.random.randint(jax.random.fold_in(key, 1), (couples,), 0, 1 << 20) % (room + 1)
    tallies = tallies.at[1:1 + 2 * couples:2].set(source_of - shifted).at[2:2 + 2 * couples:2].set(sink + shifted)
    return tallies[jax.random.permutation(jax.random.fold_in(key, 2), number_of)]


def setup_inputs(seed: int = 0) -> dict:
    streams_of = jax.random.split(jax.random.key(seed), 5)
    return {
        "tile_values": jnp.clip(jnp.exp(math.log(1.0) - 2.9996462 * jax.random.uniform(streams_of[0], (PANELS * CAP, LTILES, TILE), jnp.float32) ** level_of(streams_of[0], (PANELS * CAP, LTILES, TILE), ((0, 8),), -0.2, 0.2)), 0.049804688, 1.0).astype(jnp.bfloat16),
        "tile_ids": draw_tile_ids(jax.random.fold_in(streams_of[4], 71), 0),
        "doc_tiles": draw_doc_tiles(jax.random.fold_in(streams_of[4], 71), 0),
        "row_counts": uneven_parts(streams_of[3], PANELS, DOCS, CAP, 2).astype(jnp.int32),
    }


def reference(tile_values, tile_ids, doc_tiles, row_counts):
    capacity = tile_values.shape[0] // N_ROWS
    live_mask = jnp.arange(LTILES, dtype=jnp.int32)[None, :] < doc_tiles[:, None]
    masked = jnp.where(live_mask[:, :, None], tile_values, jnp.zeros_like(tile_values))
    run_ends = jnp.cumsum(row_counts).astype(jnp.int32)
    run_starts = (run_ends - row_counts).astype(jnp.int32)
    position = jnp.arange(DOCS, dtype=jnp.int32)
    global_ids = ((position % DOC_DEV) * N_ROWS + position // DOC_DEV).astype(jnp.int32)
    source = jnp.searchsorted(run_ends, global_ids, side="right").astype(jnp.int32)
    slot_rows = (source * capacity + (global_ids - run_starts[source])).astype(jnp.int32)
    values = masked[slot_rows]
    codes = tile_ids[slot_rows]
    holder = jnp.zeros((DOCS, VOCAB // TILE, TILE), values.dtype)
    holder = holder.at[jnp.arange(DOCS, dtype=jnp.int32)[:, None], codes].set(values)
    dense = holder.reshape(DOCS, VOCAB)
    widened = values.astype(jnp.float32)
    norms = jnp.sum(widened * widened, axis=(1, 2))

    def panel(panel_index):
        rows_here = lax.dynamic_slice_in_dim(dense, panel_index * DOC_DEV, DOC_DEV, 0)
        norms_here = lax.dynamic_slice_in_dim(norms, panel_index * DOC_DEV, DOC_DEV, 0)
        product = jnp.dot(rows_here, dense.T, preferred_element_type=jnp.float32)
        ratio = product / (norms_here[:, None] + norms[None, :] - product)
        order = ((panel_index - jnp.arange(N_ROWS, dtype=jnp.int32)) % N_ROWS).astype(jnp.int32)
        return ratio.reshape(DOC_DEV, N_ROWS, DOC_DEV)[:, order, :].reshape(DOC_DEV, DOCS)

    result = lax.map(panel, jnp.arange(N_ROWS, dtype=jnp.int32))
    return result.reshape(DOCS, DOCS)
```

```python
import functools

import jax
import jax.numpy as jnp
from jax import lax
from jax.experimental import pallas as pl
from jax.experimental.pallas import tpu as pltpu
from jax.sharding import PartitionSpec as P

MESH = pl.DeviceIdType.MESH
DOC_DEV = 64
ALONG = (((1,), (1,)), ((), ()))


def kernel(R, G, counts_hbm, tiles_hbm, ids_hbm, vals_hbm, num_ref, den_ref,
           counts_ref, tiles_ref, ids, vals, staged, inc, place, work, buf, marks, column,
           id_columns, own_norm, flat, fetch_sem, send_sem, recv_sem, deal_sem):
    cap, K, T = vals.shape
    span = R // G
    D = DOC_DEV
    Q = D // G
    A = staged.shape[1] - 1
    me = lax.axis_index("rows")
    grp = lax.axis_index("grp")
    home = span * G

    fetches = [
        pltpu.make_async_copy(src, dst, fetch_sem.at[n])
        for n, (src, dst) in enumerate(
            ((vals_hbm, vals), (ids_hbm, ids), (counts_hbm, counts_ref), (tiles_hbm, tiles_ref)))
    ]
    for fetch in fetches:
        fetch.start()

    barrier = pltpu.get_barrier_semaphore()

    def greet(row, g):
        pl.semaphore_signal(barrier, inc=1, device_id=(row, g), device_id_type=MESH)

    def greet_row(d, _):
        greet(lax.rem(me + d, R), grp)
        return 0

    lax.fori_loop(1, R, greet_row, 0)
    for e in range(1, G):
        greet(me, lax.rem(grp + e, G))

    def greet_partner(i, _):
        k = grp * span + i

        @pl.when(k != 0)
        def _():
            for g in range(G):
                greet(lax.rem(me + R - k, R), g)

        return 0

    lax.fori_loop(0, span, greet_partner, 0)

    for fetch in fetches[1:]:
        fetch.wait()

    def add_up(r, total):
        return total + jnp.where(r < me, counts_ref[r], 0)

    start = lax.fori_loop(0, R, add_up, jnp.int32(0), unroll=R <= 8)
    tile_line = lax.broadcasted_iota(jnp.int32, (K, T), 0)
    table = ids[...].astype(jnp.float32).astype(staged.dtype)
    fetches[0].wait()

    def stage(b, _):
        lag = lax.rem(start, R * G)
        first = lax.rem(b + R * grp + R * G - lag, R * G)
        for a in range(A):
            s = jnp.minimum(first + a * R * G, cap - 1)
            block = vals[s].astype(jnp.float32)
            block = jnp.where(tile_line < tiles_ref[s], block, 0.0)
            staged[b, a] = block.astype(staged.dtype)
        staged[b, A] = table
        return 0

    lax.fori_loop(0, R, stage, 0)
    pl.semaphore_wait(barrier, 2 * (R - 1) + G - 1)

    def far_first(n):
        half = lax.div(n + 1, 2)
        return R // 2 + jnp.where(lax.rem(n, 2) == 1, half, -half)

    def deal(n, _):
        row = lax.rem(me + far_first(n), R)
        pltpu.make_async_remote_copy(
            src_ref=staged.at[row], dst_ref=inc.at[me],
            send_sem=send_sem.at[0], recv_sem=deal_sem,
            device_id=(row, grp), device_id_type=MESH).start()
        return 0

    lax.fori_loop(0, R - 1, deal, 0)
    inc[me] = staged[me]

    def source_of(g):
        def look(r, carry):
            end, behind, begin = carry
            end = end + counts_ref[r]
            past = g >= end
            return (end, behind + jnp.where(past, 1, 0), jnp.where(past, end, begin))

        zero = jnp.int32(0)
        _, source, begin = lax.fori_loop(0, R, look, (zero, zero, zero), unroll=R <= 8)
        return jnp.minimum(source, R - 1), jnp.minimum(lax.div(g - begin, R * G), A - 1)

    def note(j, _):
        source, a = source_of((j * G + grp) * R + me)
        place[0, j] = source
        place[1, j] = a
        return 0

    lax.fori_loop(0, Q, note, 0)

    dealt = pltpu.make_async_remote_copy(
        src_ref=staged.at[pl.ds(0, R - 1)], dst_ref=inc.at[pl.ds(0, R - 1)],
        send_sem=send_sem.at[0], recv_sem=deal_sem,
        device_id=(me, lax.rem(grp + 1, G)), device_id_type=MESH)
    dealt.wait_recv()

    def bring(j, _):
        work[pl.ds(pl.multiple_of(j * K, K), K), :] = inc[place[0, j], place[1, j]].astype(jnp.float32)
        return 0

    lax.fori_loop(0, Q, bring, 0, unroll=8)
    for k in range(K):
        buf[home + grp, k * Q:(k + 1) * Q, :] = work[pl.ds(k, Q, stride=K), :].astype(buf.dtype)

    def outgoing(slot, row, g):
        return pltpu.make_async_remote_copy(
            src_ref=buf.at[home + grp], dst_ref=buf.at[slot],
            send_sem=send_sem.at[1], recv_sem=recv_sem.at[slot],
            device_id=(row, g), device_id_type=MESH)

    for e in range(1, G):
        outgoing(home + grp, me, lax.rem(grp + e, G)).start()

    def spread(n, _):
        d = far_first(n)
        outgoing(lax.rem(d, span) * G + grp, lax.rem(me + d, R), lax.div(d, span)).start()
        return 0

    lax.fori_loop(0, R - 1, spread, 0)

    lane = lax.broadcasted_iota(jnp.int32, (1, T), 1)
    in_order = jnp.concatenate(
        [(lax.broadcasted_iota(jnp.int32, (Q, T), 0) * G + g) * R for g in range(G)], axis=0)

    def hot(r, begin, panel):
        line = jnp.where(lane < counts_ref[r], begin + lane, -1)
        return jnp.where(in_order + panel == line, 1.0, 0.0).astype(jnp.bfloat16)

    def own_ids(r, carry):
        begin, rows = carry
        rows = rows + lax.dot_general(inc[r, A], hot(r, begin, me), ALONG,
                                      preferred_element_type=jnp.float32)
        return begin + counts_ref[r], rows

    _, rows = lax.fori_loop(0, R, own_ids, (jnp.int32(0), jnp.zeros((K, D), jnp.float32)),
                            unroll=R <= 8)
    marks[...] = jnp.concatenate([rows[:K // 2], rows[K // 2:]], axis=1)

    def partner_ids(i, _):
        panel = lax.rem(me + R - (grp * span + i), R)

        def one(r, carry):
            begin, columns = carry
            columns = columns + lax.dot_general(hot(r, begin, panel), inc[r, A], ALONG,
                                                preferred_element_type=jnp.float32)
            return begin + counts_ref[r], columns

        _, columns = lax.fori_loop(0, R, one, (jnp.int32(0), jnp.zeros((D, K), jnp.float32)),
                                   unroll=R <= 8)
        for k in range(K):
            id_columns[i, k] = jnp.broadcast_to(columns[:, k:k + 1], (D, T))
        return 0

    lax.fori_loop(0, span, partner_ids, 0)

    def arrived(slot):
        return pltpu.make_async_remote_copy(
            src_ref=buf.at[slot], dst_ref=buf.at[slot],
            send_sem=send_sem.at[1], recv_sem=recv_sem.at[slot],
            device_id=(me, lax.rem(grp + 1, G)), device_id_type=MESH)

    def norm_of(slot):
        total = jnp.zeros((Q, T), jnp.float32)
        for k in range(K):
            part = buf[slot, k * Q:(k + 1) * Q, :].astype(jnp.float32)
            total = total + part * part
        return jnp.broadcast_to(jnp.sum(total, axis=1, keepdims=True), (Q, T))

    for g in range(G):
        @pl.when(g != grp)
        def _():
            arrived(home + g).wait_recv()

        own_norm[g * Q:(g + 1) * Q, :] = norm_of(home + g)

    def compare(n, _):
        i = lax.div(n, G)
        g = lax.rem(n, G)
        k = grp * span + i

        @pl.when(k != 0)
        def _():
            arrived(n).wait_recv()

        slot = n + jnp.where(k == 0, home, 0)
        rows = buf[slot]
        sums = [jnp.zeros((Q, T), jnp.float32) for _ in range(2)]
        for p in range(K // 4):
            block = jnp.concatenate(
                [buf[home + h, j * Q:(j + 1) * Q, :]
                 for j in (2 * p, 2 * p + K // 2, 2 * p + 1, 2 * p + 1 + K // 2)
                 for h in range(G)], axis=0)
            gram = lax.dot_general(rows, block, ALONG, preferred_element_type=jnp.float32)
            for j in range(K):
                here = id_columns[i, j, pl.ds(pl.multiple_of(g * Q, Q), Q), :]
                for h in range(2):
                    part = gram[j * Q:(j + 1) * Q, h * T:(h + 1) * T]
                    same = here == marks[2 * p + h:2 * p + h + 1, :]
                    sums[h] = sums[h] + jnp.where(same, part, 0.0)
        total = sums[0] + sums[1]
        total = total + pltpu.roll(total, D, 1)
        flat[pl.ds(i * D + g, Q, stride=G), :] = jnp.where(lane < D, total, norm_of(slot))
        return 0

    lax.fori_loop(0, span * G, compare, 0)

    across = flat[...].T
    for g in range(G):
        product = across[g * Q:(g + 1) * Q]
        rest = own_norm[g * Q:(g + 1) * Q, :1] + across[D + g * Q:D + (g + 1) * Q] - product
        for c in range(span * D // T):
            num_ref[c, pl.ds(g, Q, stride=G), :] = product[:, c * T:(c + 1) * T]
            den_ref[c, pl.ds(g, Q, stride=G), :] = rest[:, c * T:(c + 1) * T]

    dealt.wait_send()
    pltpu.make_async_remote_copy(
        src_ref=buf.at[pl.ds(0, R + G - 2)], dst_ref=buf.at[pl.ds(0, R + G - 2)],
        send_sem=send_sem.at[1], recv_sem=recv_sem.at[0],
        device_id=(me, lax.rem(grp + 1, G)), device_id_type=MESH).wait_send()


def solution(mesh):
    R, G = mesh.shape["rows"], mesh.shape["grp"]
    span = R // G

    def on_device(tile_values, tile_ids, doc_tiles, row_counts):
        cap, K, T = tile_values.shape
        A = (cap + R * G - 1) // (R * G)
        Q = DOC_DEV // G
        anywhere = pl.BlockSpec(memory_space=pl.ANY)
        vmem = pl.BlockSpec(memory_space=pltpu.VMEM)
        part = pltpu.VMEM((span * DOC_DEV // T, DOC_DEV, T), jnp.float32)
        num, den = pl.pallas_call(
            functools.partial(kernel, R, G),
            out_shape=(part, part),
            in_specs=[anywhere] * 4,
            out_specs=(vmem, vmem),
            scratch_shapes=[
                pltpu.SMEM((R,), jnp.int32),
                pltpu.SMEM((cap,), jnp.int32),
                pltpu.VMEM((K, cap), jnp.int32),
                pltpu.VMEM((cap, K, T), jnp.bfloat16),
                pltpu.VMEM((R, A + 1, K, T), jnp.bfloat16),
                pltpu.VMEM((R, A + 1, K, T), jnp.bfloat16),
                pltpu.SMEM((2, Q), jnp.int32),
                pltpu.VMEM((Q * K, T), jnp.float32),
                pltpu.VMEM(((span + 1) * G, K * Q, T), jnp.bfloat16),
                pltpu.VMEM((K // 2, T), jnp.float32),
                pltpu.VMEM((DOC_DEV, T), jnp.float32),
                pltpu.VMEM((span, K, DOC_DEV, T), jnp.float32),
                pltpu.VMEM((DOC_DEV, T), jnp.float32),
                pltpu.VMEM((span * DOC_DEV, T), jnp.float32),
                pltpu.SemaphoreType.DMA((4,)),
                pltpu.SemaphoreType.DMA((2,)),
                pltpu.SemaphoreType.DMA(((span + 1) * G,)),
                pltpu.SemaphoreType.DMA,
            ],
            compiler_params=pltpu.CompilerParams(collective_id=0, has_side_effects=True),
        )(row_counts, doc_tiles, tile_ids.T, tile_values)
        return (num / den).transpose(1, 0, 2).reshape(DOC_DEV, span * DOC_DEV)

    placed = (P("rows", None, None), P("rows", None), P("rows"), P())
    return jax.shard_map(
        on_device, mesh=mesh, in_specs=placed, out_specs=P("rows", "grp"), check_vma=False
    )
```

```python
import functools

import jax
import jax.numpy as jnp
from jax import lax
from jax.experimental import pallas as pl
from jax.experimental.pallas import tpu as pltpu
from jax.sharding import PartitionSpec as P

MESH = pl.DeviceIdType.MESH
DOC_DEV = 64
ALONG = (((1,), (1,)), ((), ()))


def kernel(R, G, counts_hbm, tiles_hbm, ids_hbm, vals_hbm, num_ref, den_ref,
           counts_ref, tiles_ref, ids, vals, staged, inc, place, work, buf, own_columns, id_rows,
           own_norm, squares, parts, fold, fetch_sem, send_sem, spread_sem, recv_sem, deal_sem):
    cap, K, T = vals.shape
    span = R // G
    D = DOC_DEV
    Q = D // G
    A = staged.shape[1] - 1
    me = lax.axis_index("rows")
    grp = lax.axis_index("grp")
    peer = grp + 1 - 2 * lax.rem(grp, 2)
    home = span * G
    levels = R // 2
    level = lax.div(me, 2)
    side = lax.rem(me, 2)

    fetches = [
        pltpu.make_async_copy(src, dst, fetch_sem.at[n])
        for n, (src, dst) in enumerate(
            ((vals_hbm, vals), (ids_hbm, ids), (counts_hbm, counts_ref), (tiles_hbm, tiles_ref)))
    ]
    for fetch in fetches:
        fetch.start()

    barrier = pltpu.get_barrier_semaphore()

    def greet(row, g):
        pl.semaphore_signal(barrier, inc=1, device_id=(row, g), device_id_type=MESH)

    def greet_row(d, _):
        greet(lax.rem(me + d, R), peer)
        return 0

    lax.fori_loop(1, R, greet_row, 0)
    for e in range(1, G):
        greet(me, lax.rem(grp + e, G))

    for fetch in fetches[1:]:
        fetch.wait()

    def add_up(r, total):
        return total + jnp.where(r < me, counts_ref[r], 0)

    start = lax.fori_loop(0, R, add_up, jnp.int32(0), unroll=R <= 8)
    tile_line = lax.broadcasted_iota(jnp.int32, (K, T), 0)
    table = ids[...].astype(jnp.float32).astype(staged.dtype)
    fetches[0].wait()

    def stage(b, _):
        lag = lax.rem(start, R * G)
        first = lax.rem(b + R * jnp.where(b == me, grp, peer) + R * G - lag, R * G)
        for a in range(A):
            s = jnp.minimum(first + a * R * G, cap - 1)
            block = vals[s].astype(jnp.float32)
            block = jnp.where(tile_line < tiles_ref[s], block, 0.0)
            staged[b, a] = block.astype(staged.dtype)
        staged[b, A] = table
        return 0

    lax.fori_loop(0, R, stage, 0)
    pl.semaphore_wait(barrier, R - 1 + G - 1)

    def far_first(n, at, size):
        near = jnp.minimum(at, size - 1 - at)
        m = n - jnp.abs(size - 1 - 2 * at)
        up = jnp.where(m < 0, 2 * at < size, lax.rem(m, 2) == 0)
        away = jnp.where(m < 0, near - m, near - lax.div(m, 2))
        return at + jnp.where(up, away, -away)

    def deal(n, _):
        row = far_first(n, me, R)
        pltpu.make_async_remote_copy(
            src_ref=staged.at[row], dst_ref=inc.at[me],
            send_sem=send_sem, recv_sem=deal_sem,
            device_id=(row, peer), device_id_type=MESH).start()
        return 0

    lax.fori_loop(0, R - 1, deal, 0)
    inc[me] = staged[me]

    def source_of(g):
        def look(r, carry):
            end, behind, begin = carry
            end = end + counts_ref[r]
            past = g >= end
            return (end, behind + jnp.where(past, 1, 0), jnp.where(past, end, begin))

        zero = jnp.int32(0)
        _, source, begin = lax.fori_loop(0, R, look, (zero, zero, zero), unroll=R <= 8)
        return jnp.minimum(source, R - 1), jnp.minimum(lax.div(g - begin, R * G), A - 1)

    def note(j, _):
        source, a = source_of((j * G + grp) * R + me)
        place[0, j] = source
        place[1, j] = a
        return 0

    lax.fori_loop(0, Q, note, 0)

    dealt = pltpu.make_async_remote_copy(
        src_ref=staged.at[pl.ds(0, R - 1)], dst_ref=inc.at[pl.ds(0, R - 1)],
        send_sem=send_sem, recv_sem=deal_sem,
        device_id=(me, lax.rem(grp + 1, G)), device_id_type=MESH)
    dealt.wait_recv()

    def bring(j, _):
        work[pl.ds(pl.multiple_of(j * K, K), K), :] = inc[place[0, j], place[1, j]].astype(jnp.float32)
        return 0

    lax.fori_loop(0, Q, bring, 0, unroll=8)
    for k in range(K):
        buf[home + grp, k * Q:(k + 1) * Q, :] = work[pl.ds(k, Q, stride=K), :].astype(buf.dtype)

    def outgoing(sem, slot, row, g):
        return pltpu.make_async_remote_copy(
            src_ref=buf.at[home + grp], dst_ref=buf.at[slot],
            send_sem=spread_sem.at[sem], recv_sem=recv_sem.at[slot],
            device_id=(row, g), device_id_type=MESH)

    def to_own(e):
        return outgoing(2 * levels + e, home + grp, me, lax.rem(grp + e, G))

    def to_row(sem, row):
        k = lax.rem(row + R - me, R)
        return outgoing(sem, lax.rem(k, span) * G + grp, row, lax.div(k, span))

    def to_level(n, act):
        there = far_first(n, level, levels)
        act(to_row(n, 2 * there + side))

        @pl.when(lax.rem(grp, 2) == 1)
        def _():
            act(to_row(levels + n, 2 * there + 1 - side))

    def spread(act):
        for e in range(1, G):
            act(to_own(e))

        def each(n, _):
            to_level(n, act)
            return 0

        lax.fori_loop(0, levels - 1, each, 0)
        act(to_row(2 * levels, 2 * level + 1 - side))

    spread(lambda copy: copy.start())

    lane = lax.broadcasted_iota(jnp.int32, (1, T), 1)
    in_order = jnp.concatenate(
        [(lax.broadcasted_iota(jnp.int32, (Q, T), 0) * G + g) * R for g in range(G)], axis=0)

    def hot(r, begin, panel):
        line = jnp.where(lane < counts_ref[r], begin + lane, -1)
        return jnp.where(in_order + panel == line, 1.0, 0.0).astype(jnp.bfloat16)

    def own_ids(r, carry):
        begin, columns = carry
        columns = columns + lax.dot_general(hot(r, begin, me), inc[r, A], ALONG,
                                            preferred_element_type=jnp.float32)
        return begin + counts_ref[r], columns

    _, columns = lax.fori_loop(0, R, own_ids, (jnp.int32(0), jnp.zeros((D, K), jnp.float32)),
                               unroll=R <= 8)
    for k in range(K):
        own_columns[k] = jnp.broadcast_to(columns[:, k:k + 1], (D, T))

    within = jnp.concatenate([lax.broadcasted_iota(jnp.int32, (Q, D), 0)] * (T // Q), axis=0)
    low_of = lax.broadcasted_iota(jnp.int32, (K // 2, T), 0) * Q
    lanes = lax.broadcasted_iota(jnp.int32, (K // 2, T), 1)
    in_place = (lanes >= low_of) & (lanes < low_of + Q)

    def partner_ids(i, _):
        panel = lax.rem(me + R - (grp * span + i), R)

        def one(r, carry):
            begin, rows = carry
            rows = rows + lax.dot_general(inc[r, A], hot(r, begin, panel), ALONG,
                                          preferred_element_type=jnp.float32)
            return begin + counts_ref[r], rows

        _, rows = lax.fori_loop(0, R, one, (jnp.int32(0), jnp.zeros((K, D), jnp.float32)),
                                unroll=R <= 8)
        rows = rows.astype(jnp.bfloat16)
        for g in range(G):
            column = lax.broadcasted_iota(jnp.int32, (T, D), 1)
            pick = jnp.where(column == within + g * Q, 1.0, 0.0).astype(jnp.bfloat16)
            wide = lax.dot_general(rows, pick, ALONG, preferred_element_type=jnp.float32)
            for h in range(2):
                half = jnp.where(in_place, wide[h * K // 2:(h + 1) * K // 2], 0.0)
                id_rows[i * G + g, h:h + 1, :] = jnp.sum(half, axis=0, keepdims=True)
        return 0

    lax.fori_loop(0, span, partner_ids, 0)

    out_line = lax.broadcasted_iota(jnp.int32, (T, T), 0)
    spot = jnp.concatenate([lax.broadcasted_iota(jnp.int32, (T, Q), 1)] * (T // Q), axis=1)
    for h in range(2):
        for g in range(G):
            fold[h, :, g * T:(g + 1) * T] = jnp.where(
                out_line == spot * G + h * D + g, 1.0, 0.0).astype(fold.dtype)

    def arrived(slot):
        return pltpu.make_async_remote_copy(
            src_ref=buf.at[slot], dst_ref=buf.at[slot],
            send_sem=spread_sem.at[0], recv_sem=recv_sem.at[slot],
            device_id=(me, lax.rem(grp + 1, G)), device_id_type=MESH)

    def passing(i, g):
        k = grp * span + i + 1 - 2 * side
        return pltpu.make_async_remote_copy(
            src_ref=buf.at[i * G + g], dst_ref=buf.at[lax.rem(k, span) * G + g],
            send_sem=spread_sem.at[2 * levels + G + i * G + g],
            recv_sem=recv_sem.at[lax.rem(k, span) * G + g],
            device_id=(me + 1 - 2 * side, lax.div(k, span)), device_id_type=MESH)

    def passed(half, act):
        i = 2 * half

        @pl.when(grp * span + i != 0)
        def _():
            for g in range(0, G, 2):
                act(i, g)

    def pass_on(half, _):
        def act(i, g):
            arrived(i * G + g).wait_recv()
            passing(i, g).start()

        passed(half, act)
        return 0

    lax.fori_loop(0, span // 2, pass_on, 0)

    def squares_of(slot):
        total = jnp.zeros((Q, T), jnp.float32)
        for k in range(K):
            part = buf[slot, k * Q:(k + 1) * Q, :].astype(jnp.float32)
            total = total + part * part
        return total

    for g in range(G):
        @pl.when(g != grp)
        def _():
            arrived(home + g).wait_recv()

        own_norm[g * Q:(g + 1) * Q, :] = jnp.broadcast_to(
            jnp.sum(squares_of(home + g), axis=1, keepdims=True), (Q, T))

    def compare(i, _):
        k = grp * span + i
        base = jnp.where(k == 0, home, i * G)
        for g in range(G):
            @pl.when((lax.rem(k, 2) == 1) if g % 2 == 0 else (k != 0))
            def _():
                arrived(i * G + g).wait_recv()

        own = buf[home:home + G].reshape(G * K * Q, T)
        for g in range(G):
            gram = lax.dot_general(own, buf[base + g], ALONG, preferred_element_type=jnp.float32)
            theirs = [id_rows[i * G + g, h:h + 1, :] for h in range(2)]
            for e in range(G):
                sums = [jnp.zeros((Q, T), jnp.float32) for _ in range(2)]
                for j in range(K):
                    here = own_columns[j, e * Q:(e + 1) * Q, :]
                    for h in range(2):
                        part = gram[(e * K + j) * Q:(e * K + j + 1) * Q, h * T:(h + 1) * T]
                        sums[h] = sums[h] + jnp.where(here == theirs[h], part, 0.0)
                parts[i * G + g, e * Q:(e + 1) * Q, :] = sums[0] + sums[1]
            squares[pl.ds(i * D + g, Q, stride=G), :] = squares_of(base + g)
        return 0

    lax.fori_loop(0, span, compare, 0)

    def split(x):
        pieces = []
        for _ in range(3):
            pieces.append(x.astype(jnp.bfloat16))
            x = x - pieces[-1].astype(jnp.float32)
        return pieces

    ones = jnp.ones((D, T), jnp.bfloat16)
    for c in range(span * D // T):
        product = jnp.zeros((D, T), jnp.float32)
        for h in range(2):
            whole = jnp.concatenate([parts[(2 * c + h) * G + g] for g in range(G)], axis=1)
            for piece in split(whole):
                product = product + lax.dot_general(piece, fold[h], ALONG,
                                                    preferred_element_type=jnp.float32)
        rest = own_norm[...] - product
        for piece in split(squares[c * T:(c + 1) * T, :]):
            rest = rest + lax.dot_general(ones, piece, ALONG, preferred_element_type=jnp.float32)
        for g in range(G):
            num_ref[c, pl.ds(g, Q, stride=G), :] = product[g * Q:(g + 1) * Q]
            den_ref[c, pl.ds(g, Q, stride=G), :] = rest[g * Q:(g + 1) * Q]

    dealt.wait_send()
    spread(lambda copy: copy.wait_send())

    def finish(half, _):
        passed(half, lambda i, g: passing(i, g).wait_send())
        return 0

    lax.fori_loop(0, span // 2, finish, 0)


def solution(mesh):
    R, G = mesh.shape["rows"], mesh.shape["grp"]
    span = R // G

    def on_device(tile_values, tile_ids, doc_tiles, row_counts):
        cap, K, T = tile_values.shape
        A = (cap + R * G - 1) // (R * G)
        Q = DOC_DEV // G
        anywhere = pl.BlockSpec(memory_space=pl.ANY)
        vmem = pl.BlockSpec(memory_space=pltpu.VMEM)
        part = pltpu.VMEM((span * DOC_DEV // T, DOC_DEV, T), jnp.float32)
        num, den = pl.pallas_call(
            functools.partial(kernel, R, G),
            out_shape=(part, part),
            in_specs=[anywhere] * 4,
            out_specs=(vmem, vmem),
            scratch_shapes=[
                pltpu.SMEM((R,), jnp.int32),
                pltpu.SMEM((cap,), jnp.int32),
                pltpu.VMEM((K, cap), jnp.int32),
                pltpu.VMEM((cap, K, T), jnp.bfloat16),
                pltpu.VMEM((R, A + 1, K, T), jnp.bfloat16),
                pltpu.VMEM((R, A + 1, K, T), jnp.bfloat16),
                pltpu.SMEM((2, Q), jnp.int32),
                pltpu.VMEM((Q * K, T), jnp.float32),
                pltpu.VMEM(((span + 1) * G, K * Q, T), jnp.bfloat16),
                pltpu.VMEM((K, DOC_DEV, T), jnp.float32),
                pltpu.VMEM((span * G, 2, T), jnp.float32),
                pltpu.VMEM((DOC_DEV, T), jnp.float32),
                pltpu.VMEM((span * DOC_DEV, T), jnp.float32),
                pltpu.VMEM((span * G, DOC_DEV, T), jnp.float32),
                pltpu.VMEM((2, T, G * T), jnp.bfloat16),
                pltpu.SemaphoreType.DMA((4,)),
                pltpu.SemaphoreType.DMA,
                pltpu.SemaphoreType.DMA((R + G + span * G,)),
                pltpu.SemaphoreType.DMA(((span + 1) * G,)),
                pltpu.SemaphoreType.DMA,
            ],
            compiler_params=pltpu.CompilerParams(collective_id=0, has_side_effects=True),
        )(row_counts, doc_tiles, tile_ids.T, tile_values)
        return (num / den).transpose(1, 0, 2).reshape(DOC_DEV, span * DOC_DEV)

    placed = (P("rows", None, None), P("rows", None), P("rows"), P())
    return jax.shard_map(
        on_device, mesh=mesh, in_specs=placed, out_specs=P("rows", "grp"), check_vma=False
    )
```

```python
import functools

import jax
import jax.numpy as jnp
from jax import lax
from jax.experimental import pallas as pl
from jax.experimental.pallas import tpu as pltpu
from jax.sharding import PartitionSpec as P

MESH = pl.DeviceIdType.MESH
DOC_DEV = 64
ALONG = (((1,), (1,)), ((), ()))


def kernel(R, G, counts_hbm, tiles_hbm, ids_hbm, vals_hbm, out_ref,
           counts_ref, tiles_ref, ids, vals, staged, inc, tables, place, work, near, far,
           near_ids, far_ids, squares, found, got, flat, fetch_sem, deal_send, deal_recv,
           table_send, table_recv, spread_send, near_recv, far_recv, give_send, give_recv):
    cap, K, T = vals.shape
    span = R // G
    D = DOC_DEV
    Q = D // G
    A = staged.shape[1]
    me = lax.axis_index("rows")
    grp = lax.axis_index("grp")
    peer = grp + 1 - 2 * lax.rem(grp, 2)
    share = span // 2
    levels = R // 2
    level = lax.div(me, 2)
    side = lax.rem(me, 2)
    seat = side * G + grp

    fetches = [
        pltpu.make_async_copy(src, dst, fetch_sem.at[n])
        for n, (src, dst) in enumerate(
            ((vals_hbm, vals), (ids_hbm, ids), (counts_hbm, counts_ref), (tiles_hbm, tiles_ref)))
    ]
    for fetch in fetches:
        fetch.start()

    barrier = pltpu.get_barrier_semaphore()

    def greet(row, g):
        pl.semaphore_signal(barrier, inc=1, device_id=(row, g), device_id_type=MESH)

    def greet_row(d, _):
        greet(lax.rem(me + d, R), peer)
        return 0

    lax.fori_loop(1, R, greet_row, 0)
    for e in range(1, G):
        greet(me, lax.rem(grp + e, G))

    for fetch in fetches[1:]:
        fetch.wait()

    def add_up(r, total):
        return total + jnp.where(r < me, counts_ref[r], 0)

    start = lax.fori_loop(0, R, add_up, jnp.int32(0), unroll=R <= 8)
    tile_line = lax.broadcasted_iota(jnp.int32, (K, T), 0)
    tables[me] = ids[...].astype(jnp.float32).astype(tables.dtype)
    fetches[0].wait()

    def stage(b, _):
        lag = lax.rem(start, R * G)
        first = lax.rem(b + R * jnp.where(b == me, grp, peer) + R * G - lag, R * G)
        for a in range(A):
            s = jnp.minimum(first + a * R * G, cap - 1)
            block = vals[s].astype(jnp.float32)
            block = jnp.where(tile_line < tiles_ref[s], block, 0.0)
            staged[b, a] = block.astype(staged.dtype)
        return 0

    lax.fori_loop(0, R, stage, 0)
    pl.semaphore_wait(barrier, R - 1 + G - 1)

    def far_first(n, at, size):
        near = jnp.minimum(at, size - 1 - at)
        m = n - jnp.abs(size - 1 - 2 * at)
        up = jnp.where(m < 0, 2 * at < size, lax.rem(m, 2) == 0)
        away = jnp.where(m < 0, near - m, near - lax.div(m, 2))
        return at + jnp.where(up, away, -away)

    def deal(n, _):
        row = far_first(n, me, R)
        pltpu.make_async_remote_copy(
            src_ref=staged.at[row], dst_ref=inc.at[me],
            send_sem=deal_send, recv_sem=deal_recv,
            device_id=(row, peer), device_id_type=MESH).start()
        return 0

    lax.fori_loop(0, R - 1, deal, 0)

    def tell(n, _):
        pltpu.make_async_remote_copy(
            src_ref=tables.at[me], dst_ref=tables.at[me],
            send_sem=table_send, recv_sem=table_recv,
            device_id=(far_first(n, me, R), peer), device_id_type=MESH).start()
        return 0

    lax.fori_loop(0, R - 1, tell, 0)
    inc[me] = staged[me]

    def source_of(g):
        def look(r, carry):
            end, behind, begin = carry
            end = end + counts_ref[r]
            past = g >= end
            return (end, behind + jnp.where(past, 1, 0), jnp.where(past, end, begin))

        zero = jnp.int32(0)
        _, source, begin = lax.fori_loop(0, R, look, (zero, zero, zero), unroll=R <= 8)
        return jnp.minimum(source, R - 1), jnp.minimum(lax.div(g - begin, R * G), A - 1)

    def note(j, _):
        source, a = source_of((j * G + grp) * R + me)
        place[0, j] = source
        place[1, j] = a
        return 0

    lax.fori_loop(0, Q, note, 0)

    dealt = pltpu.make_async_remote_copy(
        src_ref=staged.at[pl.ds(0, R - 1)], dst_ref=inc.at[pl.ds(0, R - 1)],
        send_sem=deal_send, recv_sem=deal_recv,
        device_id=(me, lax.rem(grp + 1, G)), device_id_type=MESH)
    dealt.wait_recv()

    def bring(j, _):
        work[pl.ds(pl.multiple_of(j * K, K), K), :] = inc[place[0, j], place[1, j]].astype(jnp.float32)
        return 0

    lax.fori_loop(0, Q, bring, 0, unroll=8)
    for k in range(K):
        part = work[pl.ds(k, Q, stride=K), :].astype(near.dtype)
        near[seat, k * Q:(k + 1) * Q, :] = part
        far[0, k * Q:(k + 1) * Q, :] = part

    def mate(e):
        other = lax.rem(seat + e, 2 * G)
        return 2 * level + lax.div(other, G), lax.rem(other, G)

    def cousin(e):
        return lax.rem(seat + 2 * e, 2 * G)

    def to_mate(e):
        other = cousin(e)
        row = jnp.where(e == 0, me, 2 * level + lax.div(other, G))
        return pltpu.make_async_remote_copy(
            src_ref=far.at[0], dst_ref=near.at[seat],
            send_sem=spread_send.at[e], recv_sem=near_recv.at[seat],
            device_id=(row, jnp.where(e == 0, peer, lax.rem(other, G))), device_id_type=MESH)

    def pass_on(e):
        return pltpu.make_async_remote_copy(
            src_ref=near.at[cousin(e)], dst_ref=near.at[cousin(e)],
            send_sem=spread_send.at[G + e], recv_sem=near_recv.at[cousin(e)],
            device_id=(me, peer), device_id_type=MESH)

    def to_level(n):
        there = far_first(n, level, levels)
        lag = lax.rem(there + levels - level, levels)
        return pltpu.make_async_remote_copy(
            src_ref=far.at[0], dst_ref=far.at[lag],
            send_sem=spread_send.at[2 * G + n], recv_sem=far_recv.at[lag],
            device_id=(2 * there + side, grp), device_id_type=MESH)

    def spread(act):
        def each(n, _):
            act(to_level(n))
            return 0

        lax.fori_loop(0, levels - 1, each, 0)
        for e in range(G):
            act(to_mate(e))

    spread(lambda copy: copy.start())

    told = pltpu.make_async_remote_copy(
        src_ref=tables.at[pl.ds(0, R - 1)], dst_ref=tables.at[pl.ds(0, R - 1)],
        send_sem=table_send, recv_sem=table_recv,
        device_id=(me, lax.rem(grp + 1, G)), device_id_type=MESH)
    told.wait_recv()
    lane = lax.broadcasted_iota(jnp.int32, (1, T), 1)
    step = lax.broadcasted_iota(jnp.int32, (Q, T), 0) * (G * R)
    near_line = jnp.concatenate(
        [step + g * R + 2 * level + x for x in range(2) for g in range(G)], axis=0)
    far_line = jnp.concatenate(
        [step + grp * R + 2 * lax.rem(level + levels - lag, levels) + side
         for lag in range(levels)], axis=0)

    def look_up(r, carry):
        begin, rows, columns = carry
        line = jnp.where(lane < counts_ref[r], begin + lane, -1)
        near_hot = jnp.where(near_line == line, 1.0, 0.0).astype(jnp.bfloat16)
        far_hot = jnp.where(far_line == line, 1.0, 0.0).astype(jnp.bfloat16)
        rows = rows + lax.dot_general(tables[r], near_hot, ALONG,
                                      preferred_element_type=jnp.float32)
        columns = columns + lax.dot_general(far_hot, tables[r], ALONG,
                                            preferred_element_type=jnp.float32)
        return begin + counts_ref[r], rows, columns

    nothing = (jnp.int32(0), jnp.zeros((K, T), jnp.float32),
               jnp.zeros((levels * Q, K), jnp.float32))
    _, rows, columns = lax.fori_loop(0, R, look_up, nothing, unroll=R <= 8)
    near_ids[...] = rows
    for k in range(K):
        far_ids[k] = jnp.broadcast_to(columns[:, k:k + 1], (levels * Q, T))

    def squares_of(ref, slot):
        total = jnp.zeros((Q, T), jnp.float32)
        for k in range(K):
            part = ref[slot, k * Q:(k + 1) * Q, :].astype(jnp.float32)
            total = total + part * part
        return total

    def split(x):
        pieces = []
        for _ in range(3):
            pieces.append(x.astype(jnp.bfloat16))
            x = x - pieces[-1].astype(jnp.float32)
        return pieces

    def landed(slot):
        pltpu.make_async_remote_copy(
            src_ref=far.at[0], dst_ref=near.at[slot],
            send_sem=spread_send.at[0], recv_sem=near_recv.at[slot],
            device_id=(me, peer), device_id_type=MESH).wait_recv()

    for e in range(1, G):
        landed(cousin(e))
        pass_on(e).start()
    for e in range(G):
        landed(lax.rem(peer + side * G + 2 * e, 2 * G))

    for slot in range(2 * G):
        squares[slot * Q:(slot + 1) * Q, :] = squares_of(near, slot)

    ones = jnp.ones((Q, T), jnp.bfloat16)
    near_norm = jnp.zeros((Q, T), jnp.float32)
    for piece in split(squares[...]):
        near_norm = near_norm + lax.dot_general(ones, piece, ALONG,
                                                preferred_element_type=jnp.float32)

    def compare(group, _):
        rows = far[pl.ds(group * batch, batch)].reshape(batch * K * Q, T)
        sums = [[jnp.zeros((Q, T), jnp.float32) for _ in range(2)] for _ in range(batch)]
        for p in range(K // 2):
            block = jnp.concatenate(
                [near[slot, k * Q:(k + 1) * Q, :]
                 for k in (2 * p, 2 * p + 1) for slot in range(2 * G)], axis=0)
            gram = lax.dot_general(rows, block, ALONG, preferred_element_type=jnp.float32)
            theirs = [near_ids[2 * p + h:2 * p + h + 1, :] for h in range(2)]
            for b in range(batch):
                for k in range(K):
                    first = pl.multiple_of((group * batch + b) * Q, Q)
                    here = far_ids[k, pl.ds(first, Q), :]
                    for h in range(2):
                        part = gram[(b * K + k) * Q:(b * K + k + 1) * Q, h * T:(h + 1) * T]
                        sums[b][h] = sums[b][h] + jnp.where(here == theirs[h], part, 0.0)
        for b in range(batch):
            lag = group * batch + b
            product = sums[b][0] + sums[b][1]
            norm = jnp.sum(squares_of(far, lag), axis=1, keepdims=True)
            found[lag] = product / (near_norm + norm - product)
        return 0

    dealt.wait_send()
    told.wait_send()
    spread(lambda copy: copy.wait_send())

    def visit(lag, _):
        pltpu.make_async_remote_copy(
            src_ref=far.at[0], dst_ref=far.at[lag],
            send_sem=spread_send.at[0], recv_sem=far_recv.at[lag],
            device_id=mate(1), device_id_type=MESH).wait_recv()
        return 0

    lax.fori_loop(1, levels, visit, 0)
    batch = min(levels, 4)
    lax.fori_loop(0, levels // batch, compare, 0)
    found[levels] = found[0]

    def give(e):
        row, g = mate(e)
        turned = side * jnp.abs(lax.rem(row, 2) - side)
        return pltpu.make_async_remote_copy(
            src_ref=found.at[pl.ds(g * share + turned, share)], dst_ref=got.at[seat],
            send_sem=give_send.at[e], recv_sem=give_recv.at[seat],
            device_id=(row, g), device_id_type=MESH)

    for e in range(1, 2 * G):
        give(e).start()
    got[seat] = found[pl.ds(grp * share, share)]

    for slot in range(2 * G):
        @pl.when(slot != seat)
        def _():
            pltpu.make_async_remote_copy(
                src_ref=found.at[pl.ds(0, share)], dst_ref=got.at[slot],
                send_sem=give_send.at[0], recv_sem=give_recv.at[slot],
                device_id=mate(1), device_id_type=MESH).wait_recv()

        for s in range(share):
            i = 2 * s + jnp.abs(slot // G - side)
            flat[pl.ds(i * D + slot % G, Q, stride=G), :] = got[slot, s]

    across = flat[...].T
    across = jnp.where(side == 0, across[:D], across[D:])
    for g in range(G):
        for c in range(span * D // T):
            out_ref[c, pl.ds(g, Q, stride=G), :] = across[g * Q:(g + 1) * Q, c * T:(c + 1) * T]

    for e in range(1, G):
        pass_on(e).wait_send()
    for e in range(1, 2 * G):
        give(e).wait_send()


def solution(mesh):
    R, G = mesh.shape["rows"], mesh.shape["grp"]
    span = R // G

    def on_device(tile_values, tile_ids, doc_tiles, row_counts):
        cap, K, T = tile_values.shape
        A = (cap + R * G - 1) // (R * G)
        Q = DOC_DEV // G
        chunks = span * DOC_DEV // T
        anywhere = pl.BlockSpec(memory_space=pl.ANY)
        dma = pltpu.SemaphoreType.DMA
        out = pl.pallas_call(
            functools.partial(kernel, R, G),
            out_shape=pltpu.VMEM((chunks, DOC_DEV, T), jnp.float32),
            in_specs=[anywhere] * 4,
            out_specs=pl.BlockSpec(memory_space=pltpu.VMEM),
            scratch_shapes=[
                pltpu.SMEM((R,), jnp.int32),
                pltpu.SMEM((cap,), jnp.int32),
                pltpu.VMEM((K, cap), jnp.int32),
                pltpu.VMEM((cap, K, T), jnp.bfloat16),
                pltpu.VMEM((R, A, K, T), jnp.bfloat16),
                pltpu.VMEM((R, A, K, T), jnp.bfloat16),
                pltpu.VMEM((R, K, T), jnp.bfloat16),
                pltpu.SMEM((2, Q), jnp.int32),
                pltpu.VMEM((Q * K, T), jnp.float32),
                pltpu.VMEM((2 * G, K * Q, T), jnp.bfloat16),
                pltpu.VMEM((R // 2, K * Q, T), jnp.bfloat16),
                pltpu.VMEM((K, T), jnp.float32),
                pltpu.VMEM((K, R // 2 * Q, T), jnp.float32),
                pltpu.VMEM((2 * G * Q, T), jnp.float32),
                pltpu.VMEM((R // 2 + 1, Q, T), jnp.float32),
                pltpu.VMEM((2 * G, span // 2, Q, T), jnp.float32),
                pltpu.VMEM((span * DOC_DEV, T), jnp.float32),
                dma((4,)), dma, dma, dma, dma, dma((2 * G + R // 2,)), dma((2 * G,)),
                dma((R // 2,)), dma((2 * G,)), dma((2 * G,)),
            ],
            compiler_params=pltpu.CompilerParams(collective_id=0, has_side_effects=True),
        )(row_counts, doc_tiles, tile_ids.T, tile_values)
        return out.transpose(1, 0, 2).reshape(DOC_DEV, span * DOC_DEV)

    placed = (P("rows", None, None), P("rows", None), P("rows"), P())
    return jax.shard_map(
        on_device, mesh=mesh, in_specs=placed, out_specs=P("rows", "grp"), check_vma=False
    )
```

```python
import functools

import jax
import jax.numpy as jnp
from jax import lax
from jax.experimental import pallas as pl
from jax.experimental.pallas import tpu as pltpu
from jax.sharding import PartitionSpec as P

MESH = pl.DeviceIdType.MESH
DOC_DEV = 64
ALONG = (((1,), (1,)), ((), ()))


def kernel(R, G, counts_hbm, tiles_hbm, ids_hbm, vals_hbm, out_ref,
           counts_ref, tiles_ref, ids, vals, staged, inc, tables, place, work, near, far,
           near_ids, far_ids, squares, found, got, flat, fetch_sem, deal_send, deal_recv,
           table_send, table_recv, level_send, far_recv, mate_send, pass_send, near_recv,
           give_send, give_recv):
    cap, K, T = vals.shape
    span = R // G
    D = DOC_DEV
    Q = D // G
    A = staged.shape[1]
    me = lax.axis_index("rows")
    grp = lax.axis_index("grp")
    peer = grp + 1 - 2 * lax.rem(grp, 2)
    share = span // 2
    levels = R // 2
    level = lax.div(me, 2)
    side = lax.rem(me, 2)
    seat = side * G + grp

    fetches = [
        pltpu.make_async_copy(src, dst, fetch_sem.at[n])
        for n, (src, dst) in enumerate(
            ((vals_hbm, vals), (ids_hbm, ids), (counts_hbm, counts_ref), (tiles_hbm, tiles_ref)))
    ]
    for fetch in fetches:
        fetch.start()

    barrier = pltpu.get_barrier_semaphore()

    def greet(row, g):
        pl.semaphore_signal(barrier, inc=1, device_id=(row, g), device_id_type=MESH)

    def greet_row(d, _):
        greet(lax.rem(me + d, R), peer)
        return 0

    lax.fori_loop(1, R, greet_row, 0)
    for e in range(1, G):
        greet(me, lax.rem(grp + e, G))

    for fetch in fetches[1:]:
        fetch.wait()

    def add_up(r, total):
        return total + jnp.where(r < me, counts_ref[r], 0)

    start = lax.fori_loop(0, R, add_up, jnp.int32(0), unroll=R <= 8)
    tile_line = lax.broadcasted_iota(jnp.int32, (K, T), 0)
    tables[me] = ids[...].astype(jnp.float32).astype(tables.dtype)
    fetches[0].wait()

    def stage(b, _):
        lag = lax.rem(start, R * G)
        first = lax.rem(b + R * jnp.where(b == me, grp, peer) + R * G - lag, R * G)
        for a in range(A):
            s = jnp.minimum(first + a * R * G, cap - 1)
            block = vals[s].astype(jnp.float32)
            block = jnp.where(tile_line < tiles_ref[s], block, 0.0)
            staged[b, a] = block.astype(staged.dtype)
        return 0

    lax.fori_loop(0, R, stage, 0)
    pl.semaphore_wait(barrier, R - 1 + G - 1)

    def far_first(n, at, size):
        near = jnp.minimum(at, size - 1 - at)
        m = n - jnp.abs(size - 1 - 2 * at)
        up = jnp.where(m < 0, 2 * at < size, lax.rem(n, 2) == 0)
        away = jnp.where(m < 0, near - m, near - lax.div(m, 2))
        return at + jnp.where(up, away, -away)

    def farthest(n):
        there = jnp.where(n == R - 2, level, far_first(lax.div(n, 2), level, levels))
        return 2 * there + jnp.where(lax.rem(n, 2) == 0, 1 - side, side)

    def deal(n, _):
        row = farthest(n)
        pltpu.make_async_remote_copy(
            src_ref=staged.at[row], dst_ref=inc.at[me],
            send_sem=deal_send, recv_sem=deal_recv,
            device_id=(row, peer), device_id_type=MESH).start()
        return 0

    lax.fori_loop(0, R - 1, deal, 0)

    def tell(n, _):
        pltpu.make_async_remote_copy(
            src_ref=tables.at[me], dst_ref=tables.at[me],
            send_sem=table_send, recv_sem=table_recv,
            device_id=(farthest(n), peer), device_id_type=MESH).start()
        return 0

    lax.fori_loop(0, R - 1, tell, 0)
    inc[me] = staged[me]

    def source_of(g):
        def look(r, carry):
            end, behind, begin = carry
            end = end + counts_ref[r]
            past = g >= end
            return (end, behind + jnp.where(past, 1, 0), jnp.where(past, end, begin))

        zero = jnp.int32(0)
        _, source, begin = lax.fori_loop(0, R, look, (zero, zero, zero), unroll=R <= 8)
        return jnp.minimum(source, R - 1), jnp.minimum(lax.div(g - begin, R * G), A - 1)

    def note(j, _):
        source, a = source_of((j * G + grp) * R + me)
        place[0, j] = source
        place[1, j] = a
        return 0

    lax.fori_loop(0, Q, note, 0)

    dealt = pltpu.make_async_remote_copy(
        src_ref=staged.at[pl.ds(0, R - 1)], dst_ref=inc.at[pl.ds(0, R - 1)],
        send_sem=deal_send, recv_sem=deal_recv,
        device_id=(me, lax.rem(grp + 1, G)), device_id_type=MESH)
    dealt.wait_recv()

    def bring(j, _):
        work[pl.ds(pl.multiple_of(j * K, K), K), :] = inc[place[0, j], place[1, j]].astype(jnp.float32)
        return 0

    lax.fori_loop(0, Q, bring, 0, unroll=8)
    for k in range(K):
        part = work[pl.ds(k, Q, stride=K), :].astype(near.dtype)
        near[seat, k * Q:(k + 1) * Q, :] = part
        far[0, k * Q:(k + 1) * Q, :] = part

    def mate(e):
        other = lax.rem(seat + e, 2 * G)
        return 2 * level + lax.div(other, G), lax.rem(other, G)

    def cousin(e):
        return lax.rem(seat + 2 * e, 2 * G)

    def flip(slot):
        return slot + 1 - 2 * lax.rem(slot, 2)

    def to_mate(e):
        other = flip(cousin(e))
        return pltpu.make_async_remote_copy(
            src_ref=far.at[0], dst_ref=near.at[seat],
            send_sem=mate_send, recv_sem=near_recv.at[lax.rem(G - e, G)],
            device_id=(2 * level + lax.div(other, G), lax.rem(other, G)), device_id_type=MESH)

    def pass_on(e):
        return pltpu.make_async_remote_copy(
            src_ref=near.at[flip(cousin(e))], dst_ref=near.at[flip(cousin(e))],
            send_sem=pass_send, recv_sem=near_recv.at[0],
            device_id=(me, peer), device_id_type=MESH)

    def to_level(n):
        there = far_first(n, level, levels)
        lag = lax.rem(there + levels - level, levels)
        return pltpu.make_async_remote_copy(
            src_ref=far.at[0], dst_ref=far.at[lag],
            send_sem=level_send, recv_sem=far_recv.at[lag],
            device_id=(2 * there + side, peer), device_id_type=MESH)

    def spread(n, _):
        to_level(n).start()
        return 0

    lax.fori_loop(0, levels - 1, spread, 0)
    for e in range(G):
        to_mate(e).start()

    def bulk(ref, first, amount, send, recv):
        part = ref.at[pl.ds(first, amount)]
        return pltpu.make_async_remote_copy(
            src_ref=part, dst_ref=part, send_sem=send, recv_sem=recv,
            device_id=(me, peer), device_id_type=MESH)

    told = bulk(tables, 0, R - 1, table_send, table_recv)
    told.wait_recv()
    lane = lax.broadcasted_iota(jnp.int32, (1, T), 1)
    step = lax.broadcasted_iota(jnp.int32, (Q, T), 0) * (G * R)
    near_line = jnp.concatenate(
        [step + g * R + 2 * level + x for x in range(2) for g in range(G)], axis=0)
    far_line = jnp.concatenate(
        [step + (peer if lag else grp) * R + 2 * lax.rem(level + levels - lag, levels) + side
         for lag in range(levels)], axis=0)

    def look_up(r, carry):
        begin, rows, columns = carry
        line = jnp.where(lane < counts_ref[r], begin + lane, -1)
        near_hot = jnp.where(near_line == line, 1.0, 0.0).astype(jnp.bfloat16)
        far_hot = jnp.where(far_line == line, 1.0, 0.0).astype(jnp.bfloat16)
        rows = rows + lax.dot_general(tables[r], near_hot, ALONG,
                                      preferred_element_type=jnp.float32)
        columns = columns + lax.dot_general(far_hot, tables[r], ALONG,
                                            preferred_element_type=jnp.float32)
        return begin + counts_ref[r], rows, columns

    nothing = (jnp.int32(0), jnp.zeros((K, T), jnp.float32),
               jnp.zeros((levels * Q, K), jnp.float32))
    _, rows, columns = lax.fori_loop(0, R, look_up, nothing, unroll=R <= 8)
    near_ids[...] = rows
    for k in range(K):
        far_ids[k] = jnp.broadcast_to(columns[:, k:k + 1], (levels * Q, T))

    def squares_of(ref, slot):
        total = jnp.zeros((Q, T), jnp.float32)
        for k in range(K):
            part = ref[slot, k * Q:(k + 1) * Q, :].astype(jnp.float32)
            total = total + part * part
        return total

    def split(x):
        pieces = []
        for _ in range(3):
            pieces.append(x.astype(jnp.bfloat16))
            x = x - pieces[-1].astype(jnp.float32)
        return pieces

    for e in range(1, G):
        bulk(near, flip(cousin(e)), 1, mate_send, near_recv.at[e]).wait_recv()
        pass_on(e).start()
    bulk(near, 0, G, mate_send, near_recv.at[0]).wait_recv()

    for slot in range(2 * G):
        squares[slot * Q:(slot + 1) * Q, :] = squares_of(near, slot)

    ones = jnp.ones((Q, T), jnp.bfloat16)
    near_norm = jnp.zeros((Q, T), jnp.float32)
    for piece in split(squares[...]):
        near_norm = near_norm + lax.dot_general(ones, piece, ALONG,
                                                preferred_element_type=jnp.float32)

    def compare(lags):
        sums = [[jnp.zeros((Q, T), jnp.float32) for _ in range(4)] for _ in lags]
        for p in range(K // 2):
            block = jnp.concatenate(
                [near[slot, k * Q:(k + 1) * Q, :]
                 for k in (2 * p, 2 * p + 1) for slot in range(2 * G)], axis=0)
            theirs = [near_ids[2 * p + h:2 * p + h + 1, :] for h in range(2)]
            for lag, chains in zip(lags, sums):
                gram = lax.dot_general(far[lag], block, ALONG, preferred_element_type=jnp.float32)
                for k in range(K):
                    here = far_ids[k, pl.ds(pl.multiple_of(lag * Q, Q), Q), :]
                    for h in range(2):
                        part = gram[k * Q:(k + 1) * Q, h * T:(h + 1) * T]
                        c = 2 * h + k % 2
                        chains[c] = chains[c] + jnp.where(here == theirs[h], part, 0.0)
        for lag, chains in zip(lags, sums):
            product = (chains[0] + chains[1]) + (chains[2] + chains[3])
            norm = jnp.sum(squares_of(far, lag), axis=1, keepdims=True)
            found[lag] = product / (near_norm + norm - product)

    dealt.wait_send()
    told.wait_send()
    bulk(near, 0, G, mate_send, near_recv.at[0]).wait_send()
    bulk(far, 1, levels - 1, level_send, far_recv.at[0]).wait_send()

    def visitor(n):
        there = far_first(n, level, levels)
        lag = lax.rem(level + levels - there, levels)
        bulk(far, lag, 1, level_send, far_recv.at[lag]).wait_recv()
        return lag

    compare([0, visitor(levels - 2)])

    def visit(n, _):
        compare([visitor(levels - 3 - 2 * n), visitor(levels - 4 - 2 * n)])
        return 0

    lax.fori_loop(0, (levels - 2) // 2, visit, 0)
    found[levels] = found[0]

    def give(e):
        row, g = mate(e)
        turned = side * jnp.abs(lax.rem(row, 2) - side)
        return pltpu.make_async_remote_copy(
            src_ref=found.at[pl.ds(g * share + turned, share)], dst_ref=got.at[seat],
            send_sem=give_send, recv_sem=give_recv,
            device_id=(row, g), device_id_type=MESH)

    for e in range(1, 2 * G):
        give(e).start()
    got[seat] = found[pl.ds(grp * share, share)]
    bulk(near, 0, G - 1, pass_send, near_recv.at[0]).wait_send()
    given = bulk(got, 0, 2 * G - 1, give_send, give_recv)
    given.wait_send()
    given.wait_recv()

    for slot in range(2 * G):
        crossed = jnp.abs(slot // G - side)
        for s in range(share):
            lag = lax.rem(grp * share + s + slot // G * crossed, levels)
            quarter = jnp.where(lag == 0, slot % G, slot % G + 1 - 2 * (slot % 2))
            flat[pl.ds((2 * s + crossed) * D + quarter, Q, stride=G), :] = got[slot, s]

    across = flat[...].T
    across = jnp.where(side == 0, across[:D], across[D:])
    for g in range(G):
        for c in range(span * D // T):
            out_ref[c, pl.ds(g, Q, stride=G), :] = across[g * Q:(g + 1) * Q, c * T:(c + 1) * T]


def solution(mesh):
    R, G = mesh.shape["rows"], mesh.shape["grp"]
    span = R // G

    def on_device(tile_values, tile_ids, doc_tiles, row_counts):
        cap, K, T = tile_values.shape
        A = (cap + R * G - 1) // (R * G)
        Q = DOC_DEV // G
        chunks = span * DOC_DEV // T
        anywhere = pl.BlockSpec(memory_space=pl.ANY)
        dma = pltpu.SemaphoreType.DMA
        out = pl.pallas_call(
            functools.partial(kernel, R, G),
            out_shape=pltpu.VMEM((chunks, DOC_DEV, T), jnp.float32),
            in_specs=[anywhere] * 4,
            out_specs=pl.BlockSpec(memory_space=pltpu.VMEM),
            scratch_shapes=[
                pltpu.SMEM((R,), jnp.int32),
                pltpu.SMEM((cap,), jnp.int32),
                pltpu.VMEM((K, cap), jnp.int32),
                pltpu.VMEM((cap, K, T), jnp.bfloat16),
                pltpu.VMEM((R, A, K, T), jnp.bfloat16),
                pltpu.VMEM((R, A, K, T), jnp.bfloat16),
                pltpu.VMEM((R, K, T), jnp.bfloat16),
                pltpu.SMEM((2, Q), jnp.int32),
                pltpu.VMEM((Q * K, T), jnp.float32),
                pltpu.VMEM((2 * G, K * Q, T), jnp.bfloat16),
                pltpu.VMEM((R // 2, K * Q, T), jnp.bfloat16),
                pltpu.VMEM((K, T), jnp.float32),
                pltpu.VMEM((K, R // 2 * Q, T), jnp.float32),
                pltpu.VMEM((2 * G * Q, T), jnp.float32),
                pltpu.VMEM((R // 2 + 1, Q, T), jnp.float32),
                pltpu.VMEM((2 * G, span // 2, Q, T), jnp.float32),
                pltpu.VMEM((span * DOC_DEV, T), jnp.float32),
                dma((4,)), dma, dma, dma, dma, dma, dma((R // 2,)), dma, dma, dma((G,)), dma, dma,
            ],
            compiler_params=pltpu.CompilerParams(collective_id=0, has_side_effects=True),
        )(row_counts, doc_tiles, tile_ids.T, tile_values)
        return out.transpose(1, 0, 2).reshape(DOC_DEV, span * DOC_DEV)

    placed = (P("rows", None, None), P("rows", None), P("rows"), P())
    return jax.shard_map(
        on_device, mesh=mesh, in_specs=placed, out_specs=P("rows", "grp"), check_vma=False
    )
```

```python
import functools

import jax
import jax.numpy as jnp
from jax import lax
from jax.experimental import pallas as pl
from jax.experimental.pallas import tpu as pltpu
from jax.sharding import PartitionSpec as P

MESH = pl.DeviceIdType.MESH
DOC_DEV = 64
ALONG = (((1,), (1,)), ((), ()))


def kernel(R, G, counts_hbm, tiles_hbm, ids_hbm, vals_hbm, out_ref,
           counts_ref, tiles_ref, ids, vals, staged, inc, tables, place, work, near, far,
           near_ids, far_ids, squares, found, got, flat, fetch_sem, deal_send, deal_recv,
           table_send, table_recv, level_send, far_recv, mate_send, pass_send, near_recv,
           give_send, give_recv):
    cap, K, T = vals.shape
    span = R // G
    D = DOC_DEV
    Q = D // G
    A = staged.shape[1]
    me = lax.axis_index("rows")
    grp = lax.axis_index("grp")
    peer = grp + 1 - 2 * lax.rem(grp, 2)
    share = span // 2
    levels = R // 2
    level = lax.div(me, 2)
    side = lax.rem(me, 2)
    seat = side * G + grp

    fetches = [
        pltpu.make_async_copy(src, dst, fetch_sem.at[n])
        for n, (src, dst) in enumerate(
            ((vals_hbm, vals), (ids_hbm, ids), (counts_hbm, counts_ref), (tiles_hbm, tiles_ref)))
    ]
    for fetch in fetches:
        fetch.start()

    barrier = pltpu.get_barrier_semaphore()

    def greet(row, g):
        pl.semaphore_signal(barrier, inc=1, device_id=(row, g), device_id_type=MESH)

    def greet_row(d, _):
        greet(lax.rem(me + d, R), peer)
        return 0

    lax.fori_loop(1, R, greet_row, 0)
    for e in range(1, G):
        greet(me, lax.rem(grp + e, G))

    for fetch in fetches[1:]:
        fetch.wait()

    def add_up(r, total):
        return total + jnp.where(r < me, counts_ref[r], 0)

    start = lax.fori_loop(0, R, add_up, jnp.int32(0), unroll=R <= 8)
    tile_line = lax.broadcasted_iota(jnp.int32, (K, T), 0)
    tables[me] = ids[...].astype(jnp.float32).astype(tables.dtype)
    fetches[0].wait()

    def stage(b, _):
        lag = lax.rem(start, R * G)
        first = lax.rem(b + R * jnp.where(b == me, grp, peer) + R * G - lag, R * G)
        for a in range(A):
            s = jnp.minimum(first + a * R * G, cap - 1)
            block = vals[s].astype(jnp.float32)
            block = jnp.where(tile_line < tiles_ref[s], block, 0.0)
            staged[b, a] = block.astype(staged.dtype)
        return 0

    lax.fori_loop(0, R, stage, 0)
    pl.semaphore_wait(barrier, R - 1 + G - 1)

    def far_first(n, at, size):
        near = jnp.minimum(at, size - 1 - at)
        m = n - jnp.abs(size - 1 - 2 * at)
        up = jnp.where(m < 0, 2 * at < size, lax.rem(n, 2) == 0)
        away = jnp.where(m < 0, near - m, near - lax.div(m, 2))
        return at + jnp.where(up, away, -away)

    def farthest(n):
        there = jnp.where(n == R - 2, level, far_first(lax.div(n, 2), level, levels))
        return 2 * there + jnp.where(lax.rem(n, 2) == 0, 1 - side, side)

    def deal(n, _):
        row = farthest(n)
        pltpu.make_async_remote_copy(
            src_ref=staged.at[row], dst_ref=inc.at[me],
            send_sem=deal_send, recv_sem=deal_recv,
            device_id=(row, peer), device_id_type=MESH).start()
        return 0

    lax.fori_loop(0, R - 1, deal, 0)

    def tell(n, _):
        pltpu.make_async_remote_copy(
            src_ref=tables.at[me], dst_ref=tables.at[me],
            send_sem=table_send, recv_sem=table_recv,
            device_id=(farthest(n), peer), device_id_type=MESH).start()
        return 0

    lax.fori_loop(0, R - 1, tell, 0)
    inc[me] = staged[me]

    def source_of(g):
        def look(r, carry):
            end, behind, begin = carry
            end = end + counts_ref[r]
            past = g >= end
            return (end, behind + jnp.where(past, 1, 0), jnp.where(past, end, begin))

        zero = jnp.int32(0)
        _, source, begin = lax.fori_loop(0, R, look, (zero, zero, zero), unroll=R <= 8)
        return jnp.minimum(source, R - 1), jnp.minimum(lax.div(g - begin, R * G), A - 1)

    def note(j, _):
        source, a = source_of((j * G + grp) * R + me)
        place[0, j] = source
        place[1, j] = a
        return 0

    lax.fori_loop(0, Q, note, 0)

    dealt = pltpu.make_async_remote_copy(
        src_ref=staged.at[pl.ds(0, R - 1)], dst_ref=inc.at[pl.ds(0, R - 1)],
        send_sem=deal_send, recv_sem=deal_recv,
        device_id=(me, lax.rem(grp + 1, G)), device_id_type=MESH)
    dealt.wait_recv()

    def bring(j, _):
        work[pl.ds(pl.multiple_of(j * K, K), K), :] = inc[place[0, j], place[1, j]].astype(jnp.float32)
        return 0

    lax.fori_loop(0, Q, bring, 0, unroll=8)
    for k in range(K):
        part = work[pl.ds(k, Q, stride=K), :].astype(near.dtype)
        near[seat, k * Q:(k + 1) * Q, :] = part
        far[0, k * Q:(k + 1) * Q, :] = part

    def mate(e):
        other = lax.rem(seat + e, 2 * G)
        return 2 * level + lax.div(other, G), lax.rem(other, G)

    def cousin(e):
        return lax.rem(seat + 2 * e, 2 * G)

    def flip(slot):
        return slot + 1 - 2 * lax.rem(slot, 2)

    def to_mate(e):
        other = flip(cousin(e))
        return pltpu.make_async_remote_copy(
            src_ref=far.at[0], dst_ref=near.at[seat],
            send_sem=mate_send, recv_sem=near_recv.at[lax.rem(G - e, G)],
            device_id=(2 * level + lax.div(other, G), lax.rem(other, G)), device_id_type=MESH)

    def pass_on(e):
        return pltpu.make_async_remote_copy(
            src_ref=near.at[flip(cousin(e))], dst_ref=near.at[flip(cousin(e))],
            send_sem=pass_send, recv_sem=near_recv.at[0],
            device_id=(me, peer), device_id_type=MESH)

    def to_level(n):
        there = far_first(n, level, levels)
        lag = lax.rem(there + levels - level, levels)
        return pltpu.make_async_remote_copy(
            src_ref=far.at[0], dst_ref=far.at[lag],
            send_sem=level_send, recv_sem=far_recv.at[lag],
            device_id=(2 * there + side, peer), device_id_type=MESH)

    def spread(n, _):
        to_level(n).start()
        return 0

    lax.fori_loop(0, levels - 1, spread, 0)
    for e in range(G):
        to_mate(e).start()

    def bulk(ref, first, amount, send, recv):
        part = ref.at[pl.ds(first, amount)]
        return pltpu.make_async_remote_copy(
            src_ref=part, dst_ref=part, send_sem=send, recv_sem=recv,
            device_id=(me, peer), device_id_type=MESH)

    told = bulk(tables, 0, R - 1, table_send, table_recv)
    told.wait_recv()
    lane = lax.broadcasted_iota(jnp.int32, (1, T), 1)
    step = lax.broadcasted_iota(jnp.int32, (Q, T), 0) * (G * R)
    near_line = jnp.concatenate(
        [step + g * R + 2 * level + x for x in range(2) for g in range(G)], axis=0)
    far_line = jnp.concatenate(
        [step + (peer if lag else grp) * R + 2 * lax.rem(level + levels - lag, levels) + side
         for lag in range(levels)], axis=0)

    def look_up(r, carry):
        begin, rows, columns = carry
        line = jnp.where(lane < counts_ref[r], begin + lane, -1)
        near_hot = jnp.where(near_line == line, 1.0, 0.0).astype(jnp.bfloat16)
        far_hot = jnp.where(far_line == line, 1.0, 0.0).astype(jnp.bfloat16)
        rows = rows + lax.dot_general(tables[r], near_hot, ALONG,
                                      preferred_element_type=jnp.float32)
        columns = columns + lax.dot_general(far_hot, tables[r], ALONG,
                                            preferred_element_type=jnp.float32)
        return begin + counts_ref[r], rows, columns

    nothing = (jnp.int32(0), jnp.zeros((K, T), jnp.float32),
               jnp.zeros((levels * Q, K), jnp.float32))
    _, rows, columns = lax.fori_loop(0, R, look_up, nothing, unroll=R <= 8)
    near_ids[...] = rows
    for k in range(K):
        far_ids[k] = jnp.broadcast_to(columns[:, k:k + 1], (levels * Q, T))

    def squares_of(ref, slot):
        total = jnp.zeros((Q, T), jnp.float32)
        for k in range(K):
            part = ref[slot, k * Q:(k + 1) * Q, :].astype(jnp.float32)
            total = total + part * part
        return total

    def split(x):
        pieces = []
        for _ in range(3):
            pieces.append(x.astype(jnp.bfloat16))
            x = x - pieces[-1].astype(jnp.float32)
        return pieces

    for e in range(1, G):
        bulk(near, flip(cousin(e)), 1, mate_send, near_recv.at[e]).wait_recv()
        pass_on(e).start()

    def square(slot):
        squares[pl.ds(pl.multiple_of(slot * Q, Q), Q), :] = squares_of(near, slot)

    square(seat)
    for e in range(1, G):
        square(flip(cousin(e)))
    bulk(near, 0, G, mate_send, near_recv.at[0]).wait_recv()
    square(flip(seat))
    for e in range(1, G):
        square(cousin(e))

    def compare(lags, near_norm):
        sums = [[jnp.zeros((Q, T), jnp.float32) for _ in range(4)] for _ in lags]
        for p in range(K // 2):
            block = jnp.concatenate(
                [near[slot, k * Q:(k + 1) * Q, :]
                 for k in (2 * p, 2 * p + 1) for slot in range(2 * G)], axis=0)
            theirs = [near_ids[2 * p + h:2 * p + h + 1, :] for h in range(2)]
            for lag, chains in zip(lags, sums):
                gram = lax.dot_general(far[lag], block, ALONG, preferred_element_type=jnp.float32)
                for k in range(K):
                    here = far_ids[k, pl.ds(pl.multiple_of(lag * Q, Q), Q), :]
                    for h in range(2):
                        part = gram[k * Q:(k + 1) * Q, h * T:(h + 1) * T]
                        c = 2 * h + k % 2
                        chains[c] = chains[c] + jnp.where(here == theirs[h], part, 0.0)
        for lag, chains in zip(lags, sums):
            product = (chains[0] + chains[1]) + (chains[2] + chains[3])
            norm = jnp.sum(squares_of(far, lag), axis=1, keepdims=True)
            found[lag] = product / (near_norm + norm - product)

    dealt.wait_send()
    told.wait_send()
    bulk(near, 0, G, mate_send, near_recv.at[0]).wait_send()
    bulk(far, 1, levels - 1, level_send, far_recv.at[0]).wait_send()

    def visitor(n):
        there = far_first(n, level, levels)
        lag = lax.rem(level + levels - there, levels)
        bulk(far, lag, 1, level_send, far_recv.at[lag]).wait_recv()
        return lag

    distant = visitor(0)
    ones = jnp.ones((Q, T), jnp.bfloat16)
    near_norm = jnp.zeros((Q, T), jnp.float32)
    for piece in split(squares[...]):
        near_norm = near_norm + lax.dot_general(ones, piece, ALONG,
                                                preferred_element_type=jnp.float32)

    compare([0, distant], near_norm)
    found[levels] = found[0]

    def give(e, when):
        row, g = mate(e)
        first = g * share + side * jnp.abs(lax.rem(row, 2) - side)
        copy = pltpu.make_async_remote_copy(
            src_ref=found.at[pl.ds(first, share)], dst_ref=got.at[seat],
            send_sem=give_send, recv_sem=give_recv,
            device_id=(row, g), device_id_type=MESH)

        @pl.when(when(first))
        def _():
            copy.start()

    def is_early(first):
        return (share == 1) & ((lax.rem(first, levels) == 0) | (first == distant))

    for e in range(1, 2 * G):
        give(e, is_early)

    def visit(n, _):
        compare([visitor(1 + 2 * n), visitor(2 + 2 * n)], near_norm)
        return 0

    lax.fori_loop(0, (levels - 2) // 2, visit, 0)
    for e in range(1, 2 * G):
        give(e, lambda first: jnp.logical_not(is_early(first)))
    got[seat] = found[pl.ds(grp * share, share)]
    bulk(near, 0, G - 1, pass_send, near_recv.at[0]).wait_send()
    given = bulk(got, 0, 2 * G - 1, give_send, give_recv)
    given.wait_send()
    given.wait_recv()

    for slot in range(2 * G):
        crossed = jnp.abs(slot // G - side)
        for s in range(share):
            lag = lax.rem(grp * share + s + slot // G * crossed, levels)
            quarter = jnp.where(lag == 0, slot % G, slot % G + 1 - 2 * (slot % 2))
            flat[pl.ds((2 * s + crossed) * D + quarter, Q, stride=G), :] = got[slot, s]

    across = flat[...].T
    across = jnp.where(side == 0, across[:D], across[D:])
    for g in range(G):
        for c in range(span * D // T):
            out_ref[c, pl.ds(g, Q, stride=G), :] = across[g * Q:(g + 1) * Q, c * T:(c + 1) * T]


def solution(mesh):
    R, G = mesh.shape["rows"], mesh.shape["grp"]
    span = R // G

    def on_device(tile_values, tile_ids, doc_tiles, row_counts):
        cap, K, T = tile_values.shape
        A = (cap + R * G - 1) // (R * G)
        Q = DOC_DEV // G
        chunks = span * DOC_DEV // T
        anywhere = pl.BlockSpec(memory_space=pl.ANY)
        dma = pltpu.SemaphoreType.DMA
        out = pl.pallas_call(
            functools.partial(kernel, R, G),
            out_shape=pltpu.VMEM((chunks, DOC_DEV, T), jnp.float32),
            in_specs=[anywhere] * 4,
            out_specs=pl.BlockSpec(memory_space=pltpu.VMEM),
            scratch_shapes=[
                pltpu.SMEM((R,), jnp.int32),
                pltpu.SMEM((cap,), jnp.int32),
                pltpu.VMEM((K, cap), jnp.int32),
                pltpu.VMEM((cap, K, T), jnp.bfloat16),
                pltpu.VMEM((R, A, K, T), jnp.bfloat16),
                pltpu.VMEM((R, A, K, T), jnp.bfloat16),
                pltpu.VMEM((R, K, T), jnp.bfloat16),
                pltpu.SMEM((2, Q), jnp.int32),
                pltpu.VMEM((Q * K, T), jnp.float32),
                pltpu.VMEM((2 * G, K * Q, T), jnp.bfloat16),
                pltpu.VMEM((R // 2, K * Q, T), jnp.bfloat16),
                pltpu.VMEM((K, T), jnp.float32),
                pltpu.VMEM((K, R // 2 * Q, T), jnp.float32),
                pltpu.VMEM((2 * G * Q, T), jnp.float32),
                pltpu.VMEM((R // 2 + 1, Q, T), jnp.float32),
                pltpu.VMEM((2 * G, span // 2, Q, T), jnp.float32),
                pltpu.VMEM((span * DOC_DEV, T), jnp.float32),
                dma((4,)), dma, dma, dma, dma, dma, dma((R // 2,)), dma, dma, dma((G,)), dma, dma,
            ],
            compiler_params=pltpu.CompilerParams(collective_id=0, has_side_effects=True),
        )(row_counts, doc_tiles, tile_ids.T, tile_values)
        return out.transpose(1, 0, 2).reshape(DOC_DEV, span * DOC_DEV)

    placed = (P("rows", None, None), P("rows", None), P("rows"), P())
    return jax.shard_map(
        on_device, mesh=mesh, in_specs=placed, out_specs=P("rows", "grp"), check_vma=False
    )
```

```python
import functools

import jax
import jax.numpy as jnp
from jax import lax
from jax.experimental import pallas as pl
from jax.experimental.pallas import tpu as pltpu
from jax.sharding import PartitionSpec as P

MESH = pl.DeviceIdType.MESH
DOC_DEV = 64
ALONG = (((1,), (1,)), ((), ()))


def kernel(R, G, counts_hbm, tiles_hbm, ids_hbm, vals_hbm, out_ref,
           counts_ref, tiles_ref, ids, vals, staged, inc, tables, place, work, near, far,
           near_ids, far_ids, squares, mates_norm, found, got, flat, fetch_sem, deal_send, deal_recv,
           table_send, table_recv, level_send, far_recv, mate_send, pass_send, near_recv,
           give_send, give_recv):
    cap, K, T = vals.shape
    span = R // G
    D = DOC_DEV
    Q = D // G
    A = staged.shape[1]
    me = lax.axis_index("rows")
    grp = lax.axis_index("grp")
    peer = grp + 1 - 2 * lax.rem(grp, 2)
    share = span // 2
    levels = R // 2
    level = lax.div(me, 2)
    side = lax.rem(me, 2)
    seat = side * G + grp

    fetches = [
        pltpu.make_async_copy(src, dst, fetch_sem.at[n])
        for n, (src, dst) in enumerate(
            ((vals_hbm, vals), (ids_hbm, ids), (counts_hbm, counts_ref), (tiles_hbm, tiles_ref)))
    ]
    for fetch in fetches:
        fetch.start()

    barrier = pltpu.get_barrier_semaphore()

    def greet(row, g):
        pl.semaphore_signal(barrier, inc=1, device_id=(row, g), device_id_type=MESH)

    def greet_row(d, _):
        greet(lax.rem(me + d, R), peer)
        return 0

    lax.fori_loop(1, R, greet_row, 0)
    for e in range(1, G):
        greet(me, lax.rem(grp + e, G))

    for fetch in fetches[1:]:
        fetch.wait()

    def add_up(r, total):
        return total + jnp.where(r < me, counts_ref[r], 0)

    start = lax.fori_loop(0, R, add_up, jnp.int32(0), unroll=R <= 8)
    tile_line = lax.broadcasted_iota(jnp.int32, (K, T), 0)
    tables[me] = ids[...].astype(jnp.float32).astype(tables.dtype)
    fetches[0].wait()

    def stage(b, _):
        lag = lax.rem(start, R * G)
        first = lax.rem(b + R * jnp.where(b == me, grp, peer) + R * G - lag, R * G)
        for a in range(A):
            s = jnp.minimum(first + a * R * G, cap - 1)
            block = vals[s].astype(jnp.float32)
            block = jnp.where(tile_line < tiles_ref[s], block, 0.0)
            staged[b, a] = block.astype(staged.dtype)
        return 0

    lax.fori_loop(0, R, stage, 0)
    pl.semaphore_wait(barrier, R - 1 + G - 1)

    def far_first(n, at, size):
        near = jnp.minimum(at, size - 1 - at)
        m = n - jnp.abs(size - 1 - 2 * at)
        up = jnp.where(m < 0, 2 * at < size, lax.rem(n, 2) == 0)
        away = jnp.where(m < 0, near - m, near - lax.div(m, 2))
        return at + jnp.where(up, away, -away)

    def farthest(n):
        there = jnp.where(n == R - 2, level, far_first(lax.div(n, 2), level, levels))
        return 2 * there + jnp.where(lax.rem(n, 2) == 0, 1 - side, side)

    def deal(n, _):
        row = farthest(n)
        pltpu.make_async_remote_copy(
            src_ref=staged.at[row], dst_ref=inc.at[me],
            send_sem=deal_send, recv_sem=deal_recv,
            device_id=(row, peer), device_id_type=MESH).start()
        return 0

    lax.fori_loop(0, R - 1, deal, 0)

    def tell(n, _):
        pltpu.make_async_remote_copy(
            src_ref=tables.at[me], dst_ref=tables.at[me],
            send_sem=table_send, recv_sem=table_recv,
            device_id=(farthest(n), peer), device_id_type=MESH).start()
        return 0

    lax.fori_loop(0, R - 1, tell, 0)
    inc[me] = staged[me]

    def source_of(g):
        def look(r, carry):
            end, behind, begin = carry
            end = end + counts_ref[r]
            past = g >= end
            return (end, behind + jnp.where(past, 1, 0), jnp.where(past, end, begin))

        zero = jnp.int32(0)
        _, source, begin = lax.fori_loop(0, R, look, (zero, zero, zero), unroll=R <= 8)
        return jnp.minimum(source, R - 1), jnp.minimum(lax.div(g - begin, R * G), A - 1)

    def note(j, _):
        source, a = source_of((j * G + grp) * R + me)
        place[0, j] = source
        place[1, j] = a
        return 0

    lax.fori_loop(0, Q, note, 0)

    dealt = pltpu.make_async_remote_copy(
        src_ref=staged.at[pl.ds(0, R - 1)], dst_ref=inc.at[pl.ds(0, R - 1)],
        send_sem=deal_send, recv_sem=deal_recv,
        device_id=(me, lax.rem(grp + 1, G)), device_id_type=MESH)
    dealt.wait_recv()

    def bring(j, _):
        work[pl.ds(pl.multiple_of(j * K, K), K), :] = inc[place[0, j], place[1, j]].astype(jnp.float32)
        return 0

    lax.fori_loop(0, Q, bring, 0, unroll=8)
    for k in range(K):
        part = work[pl.ds(k, Q, stride=K), :].astype(near.dtype)
        near[seat, k * Q:(k + 1) * Q, :] = part
        far[0, k * Q:(k + 1) * Q, :] = part

    def mate(e):
        other = lax.rem(seat + e, 2 * G)
        return 2 * level + lax.div(other, G), lax.rem(other, G)

    def cousin(e):
        return lax.rem(seat + 2 * e, 2 * G)

    def flip(slot):
        return slot + 1 - 2 * lax.rem(slot, 2)

    def to_mate(e):
        other = flip(cousin(e))
        return pltpu.make_async_remote_copy(
            src_ref=far.at[0], dst_ref=near.at[seat],
            send_sem=mate_send, recv_sem=near_recv.at[lax.rem(G - e, G)],
            device_id=(2 * level + lax.div(other, G), lax.rem(other, G)), device_id_type=MESH)

    def pass_on(e):
        return pltpu.make_async_remote_copy(
            src_ref=near.at[flip(cousin(e))], dst_ref=near.at[flip(cousin(e))],
            send_sem=pass_send, recv_sem=near_recv.at[0],
            device_id=(me, peer), device_id_type=MESH)

    def to_level(n):
        there = far_first(n, level, levels)
        lag = lax.rem(there + levels - level, levels)
        return pltpu.make_async_remote_copy(
            src_ref=far.at[0], dst_ref=far.at[lag],
            send_sem=level_send, recv_sem=far_recv.at[lag],
            device_id=(2 * there + side, peer), device_id_type=MESH)

    def spread(n, _):
        to_level(n).start()
        return 0

    lax.fori_loop(0, levels - 1, spread, 0)
    for e in range(G):
        to_mate(e).start()

    def bulk(ref, first, amount, send, recv):
        part = ref.at[pl.ds(first, amount)]
        return pltpu.make_async_remote_copy(
            src_ref=part, dst_ref=part, send_sem=send, recv_sem=recv,
            device_id=(me, peer), device_id_type=MESH)

    told = bulk(tables, 0, R - 1, table_send, table_recv)
    told.wait_recv()
    lane = lax.broadcasted_iota(jnp.int32, (1, T), 1)
    step = lax.broadcasted_iota(jnp.int32, (Q, T), 0) * (G * R)
    near_line = jnp.concatenate(
        [step + g * R + 2 * level + x for x in range(2) for g in range(G)], axis=0)
    far_line = jnp.concatenate(
        [step + (peer if lag else grp) * R + 2 * lax.rem(level + levels - lag, levels) + side
         for lag in range(levels)], axis=0)

    def look_up(r, carry):
        begin, rows, columns = carry
        line = jnp.where(lane < counts_ref[r], begin + lane, -1)
        near_hot = jnp.where(near_line == line, 1.0, 0.0).astype(jnp.bfloat16)
        far_hot = jnp.where(far_line == line, 1.0, 0.0).astype(jnp.bfloat16)
        rows = rows + lax.dot_general(tables[r], near_hot, ALONG,
                                      preferred_element_type=jnp.float32)
        columns = columns + lax.dot_general(far_hot, tables[r], ALONG,
                                            preferred_element_type=jnp.float32)
        return begin + counts_ref[r], rows, columns

    nothing = (jnp.int32(0), jnp.zeros((K, T), jnp.float32),
               jnp.zeros((levels * Q, K), jnp.float32))
    _, rows, columns = lax.fori_loop(0, R, look_up, nothing, unroll=R <= 8)
    near_ids[...] = rows
    for k in range(K):
        far_ids[k] = jnp.broadcast_to(columns[:, k:k + 1], (levels * Q, T))

    def squares_of(ref, slot):
        total = jnp.zeros((Q, T), jnp.float32)
        for k in range(K):
            part = ref[slot, k * Q:(k + 1) * Q, :].astype(jnp.float32)
            total = total + part * part
        return total

    def split(x):
        pieces = []
        for _ in range(3):
            pieces.append(x.astype(jnp.bfloat16))
            x = x - pieces[-1].astype(jnp.float32)
        return pieces

    for e in range(1, G):
        bulk(near, flip(cousin(e)), 1, mate_send, near_recv.at[e]).wait_recv()
        pass_on(e).start()

    def square(slot):
        squares[pl.ds(pl.multiple_of(slot * Q, Q), Q), :] = squares_of(near, slot)

    square(seat)
    for e in range(1, G):
        square(flip(cousin(e)))
    bulk(near, 0, G, mate_send, near_recv.at[0]).wait_recv()
    square(flip(seat))
    for e in range(1, G):
        square(cousin(e))

    def compare(lags, norm):
        sums = [[jnp.zeros((Q, T), jnp.float32) for _ in range(4)] for _ in lags]
        for p in range(K // 2):
            block = jnp.concatenate(
                [near[slot, k * Q:(k + 1) * Q, :]
                 for k in (2 * p, 2 * p + 1) for slot in range(2 * G)], axis=0)
            theirs = [near_ids[2 * p + h:2 * p + h + 1, :] for h in range(2)]
            for lag, chains in zip(lags, sums):
                gram = lax.dot_general(far[lag], block, ALONG, preferred_element_type=jnp.float32)
                for k in range(K):
                    here = far_ids[k, pl.ds(pl.multiple_of(lag * Q, Q), Q), :]
                    for h in range(2):
                        part = gram[k * Q:(k + 1) * Q, h * T:(h + 1) * T]
                        c = 2 * h + k % 2
                        chains[c] = chains[c] + jnp.where(here == theirs[h], part, 0.0)
        near_norm = norm()
        for lag, chains in zip(lags, sums):
            product = (chains[0] + chains[1]) + (chains[2] + chains[3])
            own_norm = jnp.sum(squares_of(far, lag), axis=1, keepdims=True)
            found[lag] = product / (near_norm + own_norm - product)

    dealt.wait_send()
    told.wait_send()
    bulk(near, 0, G, mate_send, near_recv.at[0]).wait_send()
    bulk(far, 1, levels - 1, level_send, far_recv.at[0]).wait_send()

    def visitor(n):
        there = far_first(n, level, levels)
        lag = lax.rem(level + levels - there, levels)
        bulk(far, lag, 1, level_send, far_recv.at[lag]).wait_recv()
        return lag

    distant = visitor(0)
    def norm_of_mates():
        ones = jnp.ones((Q, T), jnp.bfloat16)
        total = jnp.zeros((Q, T), jnp.float32)
        for piece in split(squares[...]):
            total = total + lax.dot_general(ones, piece, ALONG, preferred_element_type=jnp.float32)
        mates_norm[...] = total
        return total

    compare([0, distant], norm_of_mates)
    found[levels] = found[0]

    def give(e, when):
        row, g = mate(e)
        first = g * share + side * jnp.abs(lax.rem(row, 2) - side)
        copy = pltpu.make_async_remote_copy(
            src_ref=found.at[pl.ds(first, share)], dst_ref=got.at[seat],
            send_sem=give_send, recv_sem=give_recv,
            device_id=(row, g), device_id_type=MESH)

        @pl.when(when(first))
        def _():
            copy.start()

    def is_early(first):
        return (share == 1) & ((lax.rem(first, levels) == 0) | (first == distant))

    for e in range(1, 2 * G):
        give(e, is_early)

    def visit(n, _):
        compare([visitor(1 + 2 * n), visitor(2 + 2 * n)], lambda: mates_norm[...])
        return 0

    lax.fori_loop(0, (levels - 2) // 2, visit, 0)
    for e in range(1, 2 * G):
        give(e, lambda first: jnp.logical_not(is_early(first)))
    got[seat] = found[pl.ds(grp * share, share)]
    bulk(near, 0, G - 1, pass_send, near_recv.at[0]).wait_send()
    given = bulk(got, 0, 2 * G - 1, give_send, give_recv)
    given.wait_send()
    given.wait_recv()

    for slot in range(2 * G):
        crossed = jnp.abs(slot // G - side)
        for s in range(share):
            lag = lax.rem(grp * share + s + slot // G * crossed, levels)
            quarter = jnp.where(lag == 0, slot % G, slot % G + 1 - 2 * (slot % 2))
            flat[pl.ds((2 * s + crossed) * D + quarter, Q, stride=G), :] = got[slot, s]

    across = flat[...].T
    across = jnp.where(side == 0, across[:D], across[D:])
    for g in range(G):
        for c in range(span * D // T):
            out_ref[c, pl.ds(g, Q, stride=G), :] = across[g * Q:(g + 1) * Q, c * T:(c + 1) * T]


def solution(mesh):
    R, G = mesh.shape["rows"], mesh.shape["grp"]
    span = R // G

    def on_device(tile_values, tile_ids, doc_tiles, row_counts):
        cap, K, T = tile_values.shape
        A = (cap + R * G - 1) // (R * G)
        Q = DOC_DEV // G
        chunks = span * DOC_DEV // T
        anywhere = pl.BlockSpec(memory_space=pl.ANY)
        dma = pltpu.SemaphoreType.DMA
        out = pl.pallas_call(
            functools.partial(kernel, R, G),
            out_shape=pltpu.VMEM((chunks, DOC_DEV, T), jnp.float32),
            in_specs=[anywhere] * 4,
            out_specs=pl.BlockSpec(memory_space=pltpu.VMEM),
            scratch_shapes=[
                pltpu.SMEM((R,), jnp.int32),
                pltpu.SMEM((cap,), jnp.int32),
                pltpu.VMEM((K, cap), jnp.int32),
                pltpu.VMEM((cap, K, T), jnp.bfloat16),
                pltpu.VMEM((R, A, K, T), jnp.bfloat16),
                pltpu.VMEM((R, A, K, T), jnp.bfloat16),
                pltpu.VMEM((R, K, T), jnp.bfloat16),
                pltpu.SMEM((2, Q), jnp.int32),
                pltpu.VMEM((Q * K, T), jnp.float32),
                pltpu.VMEM((2 * G, K * Q, T), jnp.bfloat16),
                pltpu.VMEM((R // 2, K * Q, T), jnp.bfloat16),
                pltpu.VMEM((K, T), jnp.float32),
                pltpu.VMEM((K, R // 2 * Q, T), jnp.float32),
                pltpu.VMEM((2 * G * Q, T), jnp.float32),
                pltpu.VMEM((Q, T), jnp.float32),
                pltpu.VMEM((R // 2 + 1, Q, T), jnp.float32),
                pltpu.VMEM((2 * G, span // 2, Q, T), jnp.float32),
                pltpu.VMEM((span * DOC_DEV, T), jnp.float32),
                dma((4,)), dma, dma, dma, dma, dma, dma((R // 2,)), dma, dma, dma((G,)), dma, dma,
            ],
            compiler_params=pltpu.CompilerParams(
                collective_id=0, has_side_effects=True),
        )(row_counts, doc_tiles, tile_ids.T, tile_values)
        return out.transpose(1, 0, 2).reshape(DOC_DEV, span * DOC_DEV)

    placed = (P("rows", None, None), P("rows", None), P("rows"), P())
    return jax.shard_map(
        on_device, mesh=mesh, in_specs=placed, out_specs=P("rows", "grp"), check_vma=False
    )
```
